32 devices in a mesh: gx: 4 (over z), gy: 8 (over y, x, core).
Axes of the slice: x: 2, y: 2, z: 4, core: 2. Of those that a mesh axis runs over, the one named last changes fastest.
Arguments:
- tokens: bfloat16 [2048, 7168], P(('gx', 'gy')), may hold values from -6 to 6
- expert_ids: int32 [2048, 8], P(('gx', 'gy')), may hold values from 0 to 95, all different within a row; in each aligned block of 64 rows (0 to 63, 64 to 127, ...) at most 8 rows name the same one
- router_weight: bfloat16 [7168, 96], P(None, ('gx', 'gy')), may hold values from -0.0625 to 0.0625
- gate_weight: bfloat16 [96, 7168, 128], P(('gx', 'gy')), may hold values from -0.0625 to 0.0625
- up_weight: bfloat16 [96, 7168, 128], P(('gx', 'gy')), may hold values from -0.0625 to 0.0625
- down_weight: bfloat16 [96, 128, 7168], P(('gx', 'gy')), may hold values from -0.5 to 0.5
Outputs:
- mixed: bfloat16 [2048, 7168], P(('gx', 'gy'))
The draws below stay inside these ranges and needn't reach their ends.
Inputs may be any that keep to these rules, and one draw needn't show every extreme that they name: `expert_ids`: each row names 8 different experts of 0 to 95; within each aligned block of 64 rows (the tokens of one device, in order) no expert is named more than 8 times, a bound that some block reaches; every expert is named by some row. Expert e is row e of the expert weight arrays and column e of router_weight.
All inputs are finite; a program needn't handle non-finite values.
Results may differ from the reference program's by a relative error of at most 0.0025.
Values may be sent and summed in bfloat16 or wider, within the bound.
A program may use at most 192 MiB of HBM per device.

```python
import math
import jax
import jax.numpy as jnp
import numpy as np
from jax import lax

D = 7168
TOP_K = 8
FF = 128
TOK_DEV = 64
EXPERTS = 96
TOKENS = 2048
CAP = 8
DEVICES = 32


def block_scale(rng, dims, shards, low, high):
    gain, own = 1.0, jax.random.fold_in(rng, 6)
    for dim, parts in shards:
        draws = jnp.exp(jax.random.uniform(jax.random.fold_in(own, dim), (parts,), jnp.float32, low / len(shards), high / len(shards)))
        gain = gain * jnp.repeat(draws, dims[dim] // parts).reshape([-1 if axis == dim else 1 for axis in range(len(dims))])
    return gain


def routed_block(stream_key, own, number, rows, number_of, top, most, lean):
    order = jax.random.permutation(stream_key, number_of)
    packed, ordinary = shares(number_of, rows * top, most, lean, True), shares(number_of, rows * top, most, lean, False)
    places = jnp.arange(number_of)

    def named(tallies, offset_by):
        used = int((tallies > 0).sum())
        fixed = max(1, used // 4)
        moved = fixed + (places - fixed + offset_by * (used - fixed)) % max(1, number_of - fixed)
        return jnp.zeros((number_of,), jnp.int32).at[order[jnp.where(places < fixed, places, moved)]].set(jnp.asarray(tallies, jnp.int32))

    tallies = jnp.where(number % 4 == 0, named(packed, number // 4), named(ordinary, number - number // 4 - 1))
    mixed = jax.random.permutation(jax.random.fold_in(own, 3), number_of)
    donor, receiver = mixed[0:number_of // 2 * 2:2], mixed[1:number_of // 2 * 2:2]
    room = jnp.minimum(tallies[donor] - 1, most - tallies[receiver]) // 2
    room = jnp.where((donor == order[0]) | (receiver == order[0]) | (tallies[receiver] == 0), 0, jnp.maximum(room, 0))
    moved = jax.random.randint(jax.random.fold_in(own, 4), (number_of // 2,), 0, 1 << 20) % (room + 1)
    tallies = tallies.at[donor].add(-moved).at[receiver].add(moved)
    members = jnp.searchsorted(jnp.cumsum(tallies), jnp.arange(rows * top), side="right").astype(jnp.int32)
    table = members.reshape(top, rows).T
    table = table[jax.random.permutation(jax.random.fold_in(own, 1), rows)]
    offset_by = jax.random.randint(jax.random.fold_in(own, 2), (rows, 1), 0, top)
    return jnp.take_along_axis(table, (jnp.arange(top)[None, :] + offset_by) % top, axis=1)


def shares(amount, total, bound, lean, full):
    weights = [(1 << 20) // math.isqrt(rank ** lean) + 1 for rank in range(1, amount + 1)]
    largest = bound if full else min(bound, max(-(-total // amount), total * weights[0] // sum(weights)))
    least = 1 if total - largest >= amount - 1 else 0
    holding, surplus = [largest] + [least] * (amount - 1), total - largest - least * (amount - 1)
    while surplus > 0:
        movable = [i for i in range(1, amount) if holding[i] < largest] or [i for i in range(1, amount) if holding[i] < bound]
        mass, left = sum([weights[i] for i in movable]), surplus
        for i in movable:
            extra = min(bound - holding[i], max(1, left * weights[i] // mass), surplus)
            holding[i] = holding[i] + extra
            surplus = surplus - extra
    return np.array(holding)


def gaussian(rng, shape, width, most, pieces=(), kind=jnp.bfloat16):
    factor_of = block_scale(rng, shape, pieces, -0.22, 0.18) if pieces else 1.0
    values = jax.random.normal(rng, shape, jnp.float32) * width * factor_of
    return jnp.minimum(jnp.maximum(values, -most), most).astype(kind)


def setup_inputs(seed: int = 0) -> dict:
    key_of = jax.random.split(jax.random.key(seed), 7)
    tokens = gaussian(key_of[0], (TOKENS, D), 1.0, 6.0, ((0, 32),))
    expert_ids_keys = jax.random.split(jax.random.fold_in(key_of[1], 1), TOKENS // TOK_DEV)
    expert_ids_turns = jax.random.permutation(jax.random.fold_in(key_of[1], 3), TOKENS // TOK_DEV)
    expert_ids = jax.vmap(lambda own, number: routed_block(jax.random.fold_in(key_of[1], 2), own, number, TOK_DEV, EXPERTS, TOP_K, CAP, 1))(expert_ids_keys, expert_ids_turns).reshape((TOKENS, TOP_K))
    router_weight = gaussian(key_of[2], (D, EXPERTS), D ** -0.5, 0.0625, ((1, 32),))
    gate_weight = gaussian(key_of[3], (EXPERTS, D, FF), D ** -0.5, 0.0625, ((0, 32),))
    up_weight = gaussian(key_of[4], (EXPERTS, D, FF), D ** -0.5, 0.0625, ((0, 32),))
    down_weight = gaussian(key_of[5], (EXPERTS, FF, D), FF ** -0.5, 0.5, ((0, 32),))
    return {"tokens": tokens, "expert_ids": expert_ids, "router_weight": router_weight, "gate_weight": gate_weight, "up_weight": up_weight, "down_weight": down_weight}


route_scale = 2.827
epsilon = 1e-20


def reference(tokens, expert_ids, router_weight, gate_weight, up_weight, down_weight):
    logits = jnp.dot(tokens, router_weight, preferred_element_type=jnp.float32)
    picked = jnp.take_along_axis(jax.nn.sigmoid(logits), expert_ids, axis=1)
    weights = route_scale * picked / (jnp.sum(picked, axis=1, keepdims=True) + epsilon)
    limit = DEVICES * CAP

    def visit(total, expert):
        hits = expert_ids == expert
        member = jnp.any(hits, axis=1)
        share = jnp.sum(jnp.where(hits, weights, jnp.zeros_like(weights)), axis=1)
        index = jnp.nonzero(member, size=limit, fill_value=0)[0].astype(jnp.int32)
        filled = jnp.sum(member.astype(jnp.int32))
        valid = jnp.arange(limit, dtype=jnp.int32) < filled
        chosen = tokens[index]
        gate = jnp.dot(chosen, gate_weight[expert], preferred_element_type=jnp.float32)
        upper = jnp.dot(chosen, up_weight[expert], preferred_element_type=jnp.float32)
        hidden = (jax.nn.silu(gate) * upper).astype(jnp.bfloat16)
        output = jnp.dot(hidden, down_weight[expert], preferred_element_type=jnp.float32).astype(jnp.bfloat16)
        factor = jnp.where(valid, share[index], jnp.zeros_like(share[index]))
        total = total.at[index].add(output.astype(jnp.float32) * factor[:, None])
        return total, None

    start = jnp.zeros(tokens.shape, jnp.float32)
    total, unused = lax.scan(visit, start, jnp.arange(EXPERTS, dtype=jnp.int32))
    return total.astype(jnp.bfloat16)
```

```python
import jax
import jax.numpy as jnp
from jax import lax
from jax.sharding import PartitionSpec as P

route_scale = 2.827
epsilon = 1e-20
both = ("gx", "gy")


def slots(ids, experts_wanted):
    member = jnp.any(ids[:, None, :, :] == experts_wanted[None, :, None, None], axis=3)
    member = member.astype(jnp.int32)
    rank = jnp.cumsum(member, axis=2) - member
    return member, rank


def per_device(tokens, expert_ids, router_weight, gate_weight, up_weight, down_weight):
    count, width = tokens.shape
    top = expert_ids.shape[1]
    local, _, hidden_width = gate_weight.shape
    devices = lax.axis_size(both)
    experts = local * devices
    capacity = max(1, (3 * count * top + 2 * experts - 1) // (2 * experts))
    rows_of = lax.axis_size("gx")
    columns_of = lax.axis_size("gy")
    here = lax.axis_index("gx")
    part = width // columns_of
    plane = columns_of * local

    all_tokens = lax.all_gather(tokens, both, axis=0, tiled=True)
    sliced = down_weight.reshape(local, hidden_width, columns_of, part).transpose(2, 0, 1, 3)
    down = lax.all_to_all(sliced, "gy", split_axis=0, concat_axis=0, tiled=True)
    all_ids = lax.all_gather(expert_ids, both, axis=0, tiled=False)
    router = lax.all_gather(router_weight.T, both, axis=0, tiled=True)

    near = here * plane + jnp.arange(plane, dtype=jnp.int32)
    member, rank = slots(all_ids, near)
    places = jnp.arange(capacity, dtype=jnp.int32)
    pick = (member[:, :, None, :] > 0) & (rank[:, :, None, :] == places[None, None, :, None])
    own_pick = lax.dynamic_slice_in_dim(pick, lax.axis_index("gy") * local, local, axis=1)

    gate = jnp.einsum("td,edf->tef", all_tokens, gate_weight, preferred_element_type=jnp.float32)
    upper = jnp.einsum("td,edf->tef", all_tokens, up_weight, preferred_element_type=jnp.float32)
    hidden = (jax.nn.silu(gate) * upper).astype(jnp.bfloat16)
    hidden = hidden.reshape(devices, count, local, hidden_width)
    chosen = jnp.einsum(
        "nepc,ncef->enpf", own_pick.astype(jnp.bfloat16), hidden, preferred_element_type=jnp.float32
    ).astype(jnp.bfloat16)
    chosen = lax.all_gather(chosen, "gy", axis=0, tiled=True)
    output = jnp.einsum(
        "enpf,efd->nepd",
        chosen,
        down.reshape(plane, hidden_width, part),
        preferred_element_type=jnp.float32,
    ).astype(jnp.bfloat16).reshape(devices, plane * capacity, part)

    logits = jnp.einsum("td,ed->te", all_tokens, router, preferred_element_type=jnp.float32)
    scores = jax.nn.sigmoid(logits)
    everyone = jnp.arange(experts, dtype=jnp.int32)
    hits = all_ids.reshape(-1, top)[:, :, None] == everyone
    picked = jnp.where(jnp.any(hits, axis=1), scores, 0.0)
    weights = route_scale * picked / (jnp.sum(picked, axis=1, keepdims=True) + epsilon)
    weights = lax.dynamic_slice_in_dim(weights, here * plane, plane, axis=1)
    weights = weights.reshape(devices, count, plane)
    spread = jnp.where(pick.transpose(0, 3, 1, 2), weights[:, :, :, None], 0.0)
    spread = spread.reshape(devices, count, plane * capacity)
    high = lax.reduce_precision(spread, 8, 7)
    middle = lax.reduce_precision(spread - high, 8, 7)
    low = spread - high - middle
    factors = jnp.concatenate([high, middle, low], axis=1).astype(jnp.bfloat16)
    parts = jnp.einsum("nts,nsd->ntd", factors, output, preferred_element_type=jnp.float32)
    partial = jnp.sum(parts.reshape(devices, 3, count, part), axis=1)
    total = lax.psum_scatter(partial.reshape(-1, part), "gx", scatter_dimension=0, tiled=True)
    mixed = total.astype(jnp.bfloat16).reshape(columns_of, count, part)
    mixed = lax.all_to_all(mixed, "gy", split_axis=0, concat_axis=0, tiled=True)
    return mixed.transpose(1, 0, 2).reshape(count, width)


def solution(mesh):
    placed = (
        P(both, None),
        P(both, None),
        P(None, both),
        P(both, None, None),
        P(both, None, None),
        P(both, None, None),
    )
    return jax.shard_map(
        per_device, mesh=mesh, in_specs=placed, out_specs=P(both, None), check_vma=False
    )
```
